256 devices in a mesh: samp: 4 (over y), snp: 64 (over z, x, core).
Axes of the slice: x: 4, y: 4, z: 8, core: 2. Of those that a mesh axis runs over, the one named last changes fastest.
Arguments:
- genotypes: int32 [8192, 65536], P('samp', 'snp'), may hold values from 0 to 2
- win_lo: int32 [65536], P('snp'), may hold values from 0 to 65535, as said below
- win_hi: int32 [65536], P('snp'), may hold values from 0 to 65535, as said below
- annotation: int32 [65536], P('snp'), may hold values from 0 to 127
- chromosome: int32 [65536], P('snp'), may hold values from 0 to 21, never falling along the last dimension, each value on 1 to 4096 neighbouring positions
- chi_square: float32 [65536], P('snp'), may hold values from 0.3 to 60
Outputs:
- annotation_scores: float32 [128, 65536], P('snp')
- gram: float32 [128, 128], replicated
- moments: float32 [2, 128], replicated
- totals: float32 [2], replicated
The draws below stay inside these ranges and needn't reach their ends.
Inputs may be any that keep to these rules, and one draw needn't show every extreme that they name: i - 512 <= win_lo[i] <= i, nondecreasing in i; the distance 512 is reached. i <= win_hi[i] <= i + 512, nondecreasing in i; the distance 512 is reached.
All inputs are finite; a program needn't handle non-finite values.
Results may differ from the reference program's by a relative error of at most 0.0003.
The reference program's roundings to bfloat16 on the way (of `standard`) count: a program that leaves them out, or rounds other values in their place, can miss the bound.
Values may be sent and summed in bfloat16 or wider, within the bound.
No kernel may reach another device: no remote copies, remote signals or barrier semaphores. Data moves between devices by JAX's collectives and lax.ppermute only.
A program may use at most 64 MiB of HBM per device.

```python
import math
import jax
import jax.numpy as jnp
import numpy as np
from jax import lax

A = 128
SAMPLES = 8192
SNPS = 65536
REACH = 512


def recomb_rates(key):
    base_key = jax.random.fold_in(key, 7001)
    region = jax.random.randint(jax.random.fold_in(base_key, 1), (SNPS // REACH + 1,), 1, 9)
    extra_rate = jax.random.randint(jax.random.fold_in(base_key, 2), (SNPS,), 0, 2)
    positions = jnp.arange(SNPS, dtype=jnp.int32)
    return (region[positions // REACH] + extra_rate).astype(jnp.int32)


def window_bounds(key):
    rate_steps = recomb_rates(key)
    places = jnp.cumsum(rate_steps).astype(jnp.int32)
    span_units = 3 * REACH
    lower_end = jnp.searchsorted(places, places - span_units, side='left').astype(jnp.int32)
    upper_end = (jnp.searchsorted(places, places + span_units, side='right') - 1).astype(jnp.int32)
    positions = jnp.arange(SNPS, dtype=jnp.int32)
    lower_end = jnp.maximum(lower_end, positions - REACH)
    upper_end = jnp.minimum(upper_end, positions + REACH)
    return (lower_end, upper_end)


def draw_win_lo(key, part):
    return window_bounds(key)[0]


def draw_win_hi(key, part):
    return window_bounds(key)[1]


def draw_genotypes(key, part):
    rate_steps = recomb_rates(key)
    base_key = jax.random.fold_in(key, 7003)
    frequency = jax.random.randint(jax.random.fold_in(base_key, 1), (SNPS,), 50, 500)
    keep_level = jax.random.randint(jax.random.fold_in(base_key, 4), (SNPS,), 500, 1000)
    step_keys = jax.random.split(jax.random.fold_in(base_key, 2), SNPS)
    initial = (jax.random.randint(jax.random.fold_in(base_key, 3), (2, SAMPLES), 0, 1000) < frequency[0]).astype(jnp.int32)

    def advance(haplotype, inputs):
        step_key, allele_level, flip_level, carry_level = inputs
        uniform_draws = jax.random.randint(step_key, (3, 2, SAMPLES), 0, 1000)
        fresh_allele = (uniform_draws[0] < allele_level).astype(jnp.int32)
        haplotype = jnp.where(uniform_draws[1] < flip_level, fresh_allele, haplotype)
        carried = (uniform_draws[2] < carry_level).astype(jnp.int32)
        return (haplotype, jnp.sum(haplotype * carried, 0))
    _, dosage = lax.scan(advance, initial, (step_keys, frequency, rate_steps, keep_level))
    return dosage.T.astype(jnp.int32)


def draw_chi_square(key, part):
    base_key = jax.random.fold_in(key, 7005)
    positions = jnp.arange(SNPS, dtype=jnp.float32)
    ramp = 1.0 + 2.0 * positions / SNPS
    values = jnp.exp(jax.random.uniform(base_key, (SNPS,), jnp.float32, math.log(0.3), math.log(20.0)))
    return (values * ramp).astype(jnp.float32)


def touch_ends(entries, rng, least, high):
    shape = entries.shape
    spot = [jax.random.randint(jax.random.fold_in(rng, axis), (), 0, shape[axis]) for axis in range(len(shape))]
    entries = entries.at[tuple(spot)].set(least)
    longest = shape.index(max(shape))
    spot[longest] = (spot[longest] + 1) % shape[longest]
    return entries.at[tuple(spot)].set(high)


def cumulative_ranks(number_of, lean):
    portions = [(1 << 20) // math.isqrt(rank ** lean) + 1 for rank in range(1, number_of + 1)]
    scale = 1 + sum(portions) // (1 << 30)
    return np.cumsum(np.array([max(1, weight // scale) for weight in portions]))


def ranked(stream_key, extent, number_of, lean):
    table = cumulative_ranks(number_of, lean)
    ticket = jax.random.randint(jax.random.fold_in(stream_key, 1), extent, 0, int(table[number_of - 1]))
    rank = jnp.searchsorted(jnp.asarray(table, jnp.int32), ticket, side="right")
    return jax.random.permutation(jax.random.fold_in(stream_key, 2), number_of)[rank].astype(jnp.int32)


def profile(count, total, limit, slope):
    weights = [(1 << 20) // math.isqrt(rank ** slope) + 1 for rank in range(2, count + 1)]
    surplus, holding = total - limit - (count - 1), [1] * (count - 1)
    while surplus > 0:
        free = [i for i in range(count - 1) if holding[i] < limit]
        whole, budget = sum([weights[i] for i in free]), surplus
        for i in free:
            addition = min(limit - holding[i], max(1, budget * weights[i] // whole), surplus)
            holding[i] = holding[i] + addition
            surplus = surplus - addition
    return np.array([limit] + holding)


def uneven_parts(rng, count, total, limit, lean):
    if count == 2:
        one = jax.random.randint(rng, (), max(1, total - limit), min(limit, total - 1) + 1)
        return jnp.stack([one, total - one])
    sizes = jnp.asarray(profile(count, total, limit, lean), jnp.int32)
    couples = (count - 1) // 2
    giver, sink = sizes[1:1 + 2 * couples:2], sizes[2:2 + 2 * couples:2]
    slack = jnp.minimum(giver - 1, limit - sink)
    shifted = jax.random.randint(jax.random.fold_in(rng, 1), (couples,), 0, 1 << 20) % (slack + 1)
    sizes = sizes.at[1:1 + 2 * couples:2].set(giver - shifted).at[2:2 + 2 * couples:2].set(sink + shifted)
    return sizes[jax.random.permutation(jax.random.fold_in(rng, 2), count)]


def setup_inputs(seed: int = 0) -> dict:
    key_of = jax.random.split(jax.random.key(seed), 7)
    genotypes = draw_genotypes(jax.random.fold_in(key_of[6], 71), 0)
    win_lo = draw_win_lo(jax.random.fold_in(key_of[6], 71), 0)
    win_hi = draw_win_hi(jax.random.fold_in(key_of[6], 71), 0)
    annotation = touch_ends(ranked(key_of[3], (SNPS,), A, 1), jax.random.fold_in(key_of[3], 3), 0, A - 1).astype(jnp.int32)
    chromosome = jnp.searchsorted(jnp.cumsum(uneven_parts(key_of[4], 22, SNPS, SNPS // 16, 1)), jnp.arange(SNPS), side="right").astype(jnp.int32)
    chi_square = draw_chi_square(jax.random.fold_in(key_of[6], 71), 0)
    return dict(genotypes=genotypes, win_lo=win_lo, win_hi=win_hi, annotation=annotation, chromosome=chromosome, chi_square=chi_square)


def reference(genotypes, win_lo, win_hi, annotation, chromosome, chi_square):
    dosage = genotypes.astype(jnp.float32)
    mean_dose = lax.optimization_barrier(jnp.sum(dosage, 0)) / SAMPLES
    variance = lax.optimization_barrier(jnp.sum(dosage * dosage, 0)) / SAMPLES - mean_dose * mean_dose
    standard = ((dosage - mean_dose) * lax.rsqrt(variance + 1e-05)).astype(jnp.bfloat16)
    padded = jnp.pad(standard, ((0, 0), (REACH, REACH)))
    annot_pad = jnp.pad(annotation, REACH)
    chrom_pad = jnp.pad(chromosome, REACH)
    labels = jnp.arange(A, dtype=jnp.int32)

    def one_block(block):
        first_row = (block * REACH).astype(jnp.int32)
        rows_z = lax.dynamic_slice_in_dim(standard, first_row, REACH, 1).astype(jnp.float32)
        cols_z = lax.dynamic_slice_in_dim(padded, first_row, 3 * REACH, 1).astype(jnp.float32)
        tile = lax.dot_general(rows_z, cols_z, (((0,), (0,)), ((), ())), preferred_element_type=jnp.float32)
        corr = tile / SAMPLES
        square = corr * corr
        adjusted = square - (1.0 - square) / (SAMPLES - 2)
        col_ids = first_row - REACH + jnp.arange(3 * REACH, dtype=jnp.int32)
        lower_end = lax.dynamic_slice_in_dim(win_lo, first_row, REACH)
        upper_end = lax.dynamic_slice_in_dim(win_hi, first_row, REACH)
        chrom_rows = lax.dynamic_slice_in_dim(chromosome, first_row, REACH)
        chrom_cols = lax.dynamic_slice_in_dim(chrom_pad, first_row, 3 * REACH)
        annot_cols = lax.dynamic_slice_in_dim(annot_pad, first_row, 3 * REACH)
        inside = (col_ids[None, :] >= lower_end[:, None]) & (col_ids[None, :] <= upper_end[:, None])
        inside = inside & (chrom_cols[None, :] == chrom_rows[:, None])
        kept = jnp.where(inside, adjusted, 0.0)
        member = (annot_cols[:, None] == labels[None, :]).astype(jnp.float32)
        return lax.dot_general(member, kept, (((0,), (1,)), ((), ())), precision=lax.Precision.HIGHEST, preferred_element_type=jnp.float32)
    blocks = lax.map(one_block, jnp.arange(SNPS // REACH, dtype=jnp.int32))
    scores = jnp.transpose(blocks, (1, 0, 2)).reshape(A, SNPS)
    weights = 1.0 / lax.optimization_barrier(jnp.sum(scores, 0))
    weighted = scores * weights[None, :]
    scale = A / SNPS
    gram = scale * lax.dot_general(weighted, scores, (((1,), (1,)), ((), ())), precision=lax.Precision.HIGHEST, preferred_element_type=jnp.float32)
    moments = scale * jnp.stack([lax.optimization_barrier(jnp.sum(weighted, 1)), lax.optimization_barrier(jnp.sum(weighted * chi_square[None, :], 1))])
    totals = jnp.stack([jnp.sum(weights), jnp.sum(weights * chi_square)]) / SNPS
    return (scores, gram, moments, totals)
```

```python
import functools

import jax
import jax.numpy as jnp
from jax import lax
from jax.experimental import pallas as pl
from jax.experimental.pallas import tpu as pltpu
from jax.sharding import PartitionSpec as P

A = 128
FIXED = 32000.0


def exchange(array, axis):
    return lax.all_to_all(array, axis, 0, 0, tiled=True)


def to_all(array, axis):
    size = lax.axis_size(axis)
    return exchange(jnp.broadcast_to(array[None], (size, *array.shape)), axis)


def shifted(array, axis, step):
    size = lax.axis_size(axis)
    return lax.ppermute(array, axis, [(i, (i + step) % size) for i in range(size)])


def samp_total(array):
    near, far, back = [shifted(array, "samp", step) for step in (1, 2, 3)]
    return (array + far) + (near + back)


def from_left(array, axis):
    count = lax.axis_size(axis)
    return lax.ppermute(array, axis, [(i, i + 1) for i in range(count - 1)])


def from_right(array, axis):
    count = lax.axis_size(axis)
    return lax.ppermute(array, axis, [(i + 1, i) for i in range(count - 1)])


def gram_of(rows, cols):
    return lax.dot_general(rows, cols, (((0,), (0,)), ((), ())), preferred_element_type=jnp.float32)


def count_kernel(genotypes, lower, upper, sums, held, arrived):
    rows, cols = genotypes.shape
    slots, step, _ = held.shape
    half = cols // 2
    steps = rows // step

    def load(index):
        return pltpu.make_async_copy(
            genotypes.at[pl.ds(index * step, step), :],
            held.at[index % slots],
            arrived.at[index % slots],
        )

    for index in range(slots):
        load(index).start()
    plain = jnp.zeros((8, cols), jnp.float32)
    squared = jnp.zeros((8, cols), jnp.float32)
    for index in range(steps):
        load(index).wait()
        wide = held[index % slots].astype(jnp.float32)
        narrow = wide.astype(jnp.bfloat16)
        lower[index * step : (index + 1) * step, :] = narrow[:, :half]
        upper[index * step : (index + 1) * step, :] = narrow[:, half:]
        folded = wide.reshape(step // 8, 8, cols)
        plain += jnp.sum(folded, 0)
        squared += jnp.sum(folded * folded, 0)
        if index + slots < steps:
            load(index + slots).start()
    sums[0:1, :] = jnp.sum(plain, 0, keepdims=True)
    sums[1:2, :] = jnp.sum(squared, 0, keepdims=True)


def counted(genotypes):
    rows, cols = genotypes.shape
    step = rows // 16
    half = jax.ShapeDtypeStruct((rows, cols // 2), jnp.bfloat16)
    return pl.pallas_call(
        count_kernel,
        out_shape=(half, half, jax.ShapeDtypeStruct((2, cols), jnp.float32)),
        in_specs=[pl.BlockSpec(memory_space=pl.ANY)],
        out_specs=(pl.BlockSpec(memory_space=pltpu.VMEM),) * 3,
        scratch_shapes=[pltpu.VMEM((4, step, cols), jnp.int32), pltpu.SemaphoreType.DMA((4,))],
        compiler_params=pltpu.CompilerParams(vmem_limit_bytes=57 * 2**20),
        name="counted",
    )(genotypes)


def score_kernel(total_samples, *refs):
    near, far, noted, bounds, out = refs[:4], refs[4:8], refs[8:11], refs[11:14], refs[14]
    share, reach = near[0].shape[0] // 3, near[0].shape[1]
    me = lax.axis_index("samp")
    first = lax.axis_index("snp") * (2 * reach)
    blocks = reach // share

    def summed(parts, begin, size):
        held = [part[begin : begin + size, :].astype(jnp.int32) for part in parts]
        return (held[0] + held[1] + held[2] + held[3]).astype(jnp.float32) * (1.0 / FIXED)

    def column(row):
        return jnp.transpose(jnp.broadcast_to(row, (share, share)))[:, 0:1]

    row_id = lax.broadcasted_iota(jnp.int32, (share, reach), 0) + me * share
    col_id = lax.broadcasted_iota(jnp.int32, (share, reach), 1)
    own_0, own_1 = summed(near, 0, share), summed(near, share, share)
    mixed, outer = summed(near, 2 * share, share), summed(far, 0, share)
    edge = column(summed(far, share, 8)[0:1, :share])
    outer_1 = jnp.where(row_id == col_id, edge, outer)
    cat_id = lax.broadcasted_iota(jnp.int32, (A, reach), 0).astype(jnp.float32)
    left, here, right = noted
    sides = [
        (left[0:1, :], left[1:2, :]),
        (here[0:1, :reach], here[1:2, :reach]),
        (here[0:1, reach:], here[1:2, reach:]),
        (right[0:1, :], right[1:2, :]),
    ]
    members = [(annot == cat_id).astype(jnp.bfloat16) for annot, _ in sides]
    scores, chis = [], []
    for half, parts in enumerate(((outer, own_0, mixed), (mixed, own_1, outer_1))):
        at = half * blocks + me
        low, high = [column(ref[pl.ds(at, 1), :]) for ref in bounds[:2]]
        chis.append(bounds[2][pl.ds(at, 1), :])
        start = pl.multiple_of(half * reach + me * share, share)
        chrom = column(here[1:2, pl.ds(start, share)])
        total = jnp.zeros((A, share), jnp.float32)
        for side, corr in enumerate(parts, half):
            square = corr * corr
            adjusted = square - (1.0 - square) / (total_samples - 2)
            ids = first + (side - 1) * reach + col_id
            inside = (ids >= low) & (ids <= high) & (sides[side][1] == chrom)
            rest = jnp.where(inside, adjusted, 0.0)
            for _ in range(3):
                piece = rest.astype(jnp.bfloat16)
                rest = rest - piece.astype(jnp.float32)
                total += lax.dot_general(
                    members[side],
                    piece,
                    (((1,), (1,)), ((), ())),
                    preferred_element_type=jnp.float32,
                )
        scores.append(total)
    score = jnp.concatenate(scores, 1)
    chi = jnp.concatenate(chis, 1)
    weights = 1.0 / jnp.sum(score, 0, keepdims=True)
    weighted = score * weights
    out[:, : 2 * share] = score
    out[:, 2 * share : 2 * share + A] = lax.dot_general(
        weighted,
        score,
        (((1,), (1,)), ((), ())),
        precision=lax.Precision.HIGHEST,
        preferred_element_type=jnp.float32,
    )
    lane = lax.broadcasted_iota(jnp.int32, (A, A), 1)
    plain = jnp.sum(weighted, 1, keepdims=True)
    scaled = jnp.sum(weighted * chi, 1, keepdims=True)
    all_weights = jnp.sum(weights, 1, keepdims=True)
    all_scaled = jnp.sum(weights * chi, 1, keepdims=True)
    out[:, 2 * share + A :] = jnp.where(
        lane == 0,
        plain,
        jnp.where(
            lane == 1,
            scaled,
            jnp.where(lane == 2, all_weights, jnp.where(lane == 3, all_scaled, 0.0)),
        ),
    )


def scored(near, far, noted, bounds, total_samples):
    share = near[0].shape[0] // 3
    operands = [*near, *far, *noted, *bounds]
    return pl.pallas_call(
        functools.partial(score_kernel, total_samples),
        out_shape=jax.ShapeDtypeStruct((A, 2 * share + 2 * A), jnp.float32),
        in_specs=[pl.BlockSpec(memory_space=pltpu.VMEM)] * len(operands),
        out_specs=pl.BlockSpec(memory_space=pltpu.VMEM),
        compiler_params=pltpu.CompilerParams(vmem_limit_bytes=16 * 2**20),
        cost_estimate=pl.CostEstimate(flops=2 * 10**9, bytes_accessed=2 * 10**6, transcendentals=0),
        name="scored",
    )(*operands)


def whole_step(genotypes, win_lo, win_hi, annotation, chromosome, chi_square):
    samp_rows, block_cols = genotypes.shape
    reach = block_cols // 2
    samp_count = lax.axis_size("samp")
    snp_count = lax.axis_size("snp")
    total_samples = samp_rows * samp_count
    snp_total = block_cols * snp_count
    share = reach // samp_count
    me_samp = lax.axis_index("samp")
    cats = A // snp_count

    lower, upper, sums = counted(genotypes)
    raw_left = from_left(upper, "snp")
    raw_right = from_right(lower, "snp")
    sums = samp_total(sums)
    mean_dose = sums[0] / total_samples
    variance = sums[1] / total_samples - mean_dose * mean_dose
    inverse = lax.rsqrt(variance + 1e-05)

    def standard_of(raw, mean, inv):
        return ((raw.astype(jnp.float32) - mean) * inv).astype(jnp.bfloat16)

    notes = jnp.stack(
        [annotation.astype(jnp.float32), chromosome.astype(jnp.float32), mean_dose, inverse]
    )
    z0 = standard_of(lower, mean_dose[:reach], inverse[:reach])
    z1 = standard_of(upper, mean_dose[reach:], inverse[reach:])
    z0, z1 = lax.optimization_barrier((z0, z1))
    a_id = lax.broadcasted_iota(jnp.int32, (reach, reach), 0)
    b_id = lax.broadcasted_iota(jnp.int32, (reach, reach), 1)

    def fixed(part):
        return jnp.round(part * (FIXED / total_samples)).astype(jnp.int16)

    def turned(parts):
        return [
            lax.dynamic_index_in_dim(parts, (me_samp + step) % samp_count, 0, keepdims=False)
            for step in range(samp_count)
        ]

    def shares(square):
        return square.reshape(samp_count, share, reach)

    near = jnp.concatenate(
        [
            shares(fixed(gram_of(z0, z0))),
            shares(fixed(gram_of(z1, z1))),
            shares(fixed(jnp.where(b_id <= a_id, gram_of(z0, z1), gram_of(z1, z0)))),
        ],
        1,
    )
    near = turned(near)
    near = [near[0]] + [shifted(near[step], "samp", step) for step in range(1, samp_count)]
    notes_left = from_left(notes[:, reach:], "snp")
    notes_right = from_right(notes[:, :reach], "snp")

    z_left = standard_of(raw_left, notes_left[2], notes_left[3])
    z_right = standard_of(raw_right, notes_right[2], notes_right[3])
    right_part = gram_of(z1, z_right)
    edge = jnp.sum(jnp.where(a_id == b_id, right_part, 0.0), 0)
    edge_rows = jnp.zeros((samp_count, 8, reach), jnp.int16)
    edge_rows = edge_rows.at[:, 0, :share].set(fixed(edge).reshape(samp_count, share))
    far = jnp.concatenate(
        [
            shares(fixed(jnp.where(b_id >= a_id, gram_of(z0, z_left), right_part))),
            edge_rows,
        ],
        1,
    )
    far = turned(far)
    far = [far[0]] + [shifted(far[step], "samp", step) for step in range(1, samp_count)]
    near, far, win_lo, win_hi, chi_square = lax.optimization_barrier(
        (near, far, win_lo, win_hi, chi_square)
    )

    grid_of = lambda vector: vector.reshape(-1, share)
    mine = scored(
        near,
        far,
        (notes_left, notes, notes_right),
        (grid_of(win_lo), grid_of(win_hi), grid_of(chi_square)),
        total_samples,
    )
    mine = mine.reshape(snp_count, cats, 2 * share + 2 * A)
    mine = exchange(mine, "snp")
    sums_part = jnp.sum(mine[:, :, 2 * share :], 0)
    score_part = jnp.moveaxis(mine[:, :, : 2 * share], 0, 1).reshape(cats, -1)
    sums_part = samp_total(sums_part)
    sums_whole = to_all(sums_part, "snp").reshape(A, 2 * A)
    parts = [score_part] + [shifted(score_part, "samp", step) for step in range(1, samp_count)]
    turns = jnp.stack([parts[-turn % samp_count] for turn in range(1, 2 * samp_count)])
    both = lax.dynamic_slice_in_dim(turns, samp_count - 1 - me_samp, samp_count, 0)
    split = both.reshape(samp_count, cats, snp_count, 2, share)
    regrouped = jnp.transpose(split, (1, 2, 3, 0, 4)).reshape(cats, snp_total)
    scale = A / snp_total
    gram = scale * sums_whole[:, :A]
    moments = scale * sums_whole[:, A : A + 2].T
    totals = sums_whole[0, A + 2 : A + 4] / snp_total
    return (regrouped, gram, moments, totals)


def solution(mesh):
    in_specs = (P("samp", "snp"), P("snp"), P("snp"), P("snp"), P("snp"), P("snp"))
    out_specs = (P("snp", None), P(), P(), P())
    return jax.shard_map(whole_step, mesh=mesh, in_specs=in_specs, out_specs=out_specs, check_vma=False)
```

```python
import functools

import jax
import jax.numpy as jnp
from jax import lax
from jax.experimental import pallas as pl
from jax.experimental.pallas import tpu as pltpu
from jax.sharding import PartitionSpec as P

A = 128
FIXED = 32000.0


def exchange(array, axis):
    return lax.all_to_all(array, axis, 0, 0, tiled=True)


def to_all(array, axis):
    size = lax.axis_size(axis)
    return exchange(jnp.broadcast_to(array[None], (size, *array.shape)), axis)


def shifted(array, axis, step):
    size = lax.axis_size(axis)
    return lax.ppermute(array, axis, [(i, (i + step) % size) for i in range(size)])


def samp_total(array):
    near, far, back = [shifted(array, "samp", step) for step in (1, 2, 3)]
    return (array + far) + (near + back)


def from_left(array, axis):
    count = lax.axis_size(axis)
    return lax.ppermute(array, axis, [(i, i + 1) for i in range(count - 1)])


def from_right(array, axis):
    count = lax.axis_size(axis)
    return lax.ppermute(array, axis, [(i + 1, i) for i in range(count - 1)])


def gram_of(rows, cols):
    return lax.dot_general(rows, cols, (((0,), (0,)), ((), ())), preferred_element_type=jnp.float32)


def count_kernel(genotypes, lower, upper, sums, held, arrived):
    rows, cols = genotypes.shape
    slots, step, _ = held.shape
    half = cols // 2
    steps = rows // step

    def load(index):
        return pltpu.make_async_copy(
            genotypes.at[pl.ds(index * step, step), :],
            held.at[index % slots],
            arrived.at[index % slots],
        )

    for index in range(slots):
        load(index).start()
    plain = jnp.zeros((8, cols), jnp.float32)
    squared = jnp.zeros((8, cols), jnp.float32)
    for index in range(steps):
        load(index).wait()
        wide = held[index % slots].astype(jnp.float32)
        narrow = wide.astype(jnp.bfloat16)
        lower[index * step : (index + 1) * step, :] = narrow[:, :half]
        upper[index * step : (index + 1) * step, :] = narrow[:, half:]
        folded = wide.reshape(step // 8, 8, cols)
        plain += jnp.sum(folded, 0)
        squared += jnp.sum(folded * folded, 0)
        if index + slots < steps:
            load(index + slots).start()
    sums[0:1, :] = jnp.sum(plain, 0, keepdims=True)
    sums[1:2, :] = jnp.sum(squared, 0, keepdims=True)


def counted(genotypes):
    rows, cols = genotypes.shape
    step = rows // 16
    half = pltpu.VMEM((rows, cols // 2), jnp.bfloat16)
    return pl.pallas_call(
        count_kernel,
        out_shape=(half, half, jax.ShapeDtypeStruct((2, cols), jnp.float32)),
        in_specs=[pl.BlockSpec(memory_space=pl.ANY)],
        out_specs=(pl.BlockSpec(memory_space=pltpu.VMEM),) * 3,
        scratch_shapes=[pltpu.VMEM((4, step, cols), jnp.int32), pltpu.SemaphoreType.DMA((4,))],
        compiler_params=pltpu.CompilerParams(vmem_limit_bytes=54 * 2**20),
        name="counted",
    )(genotypes)


def score_kernel(total_samples, *refs):
    near, far, noted, bounds, out = refs[:4], refs[4:8], refs[8:11], refs[11:14], refs[14]
    share, reach = near[0].shape[0] // 3, near[0].shape[1]
    me = lax.axis_index("samp")
    first = lax.axis_index("snp") * (2 * reach)
    blocks = reach // share

    def summed(parts, begin, size):
        held = [part[begin : begin + size, :].astype(jnp.int32) for part in parts]
        return (held[0] + held[1] + held[2] + held[3]).astype(jnp.float32) * (1.0 / FIXED)

    def column(row):
        return jnp.transpose(jnp.broadcast_to(row, (share, share)))[:, 0:1]

    row_id = lax.broadcasted_iota(jnp.int32, (share, reach), 0) + me * share
    col_id = lax.broadcasted_iota(jnp.int32, (share, reach), 1)
    own_0, own_1 = summed(near, 0, share), summed(near, share, share)
    mixed, outer = summed(near, 2 * share, share), summed(far, 0, share)
    edge = column(summed(far, share, 8)[0:1, :share])
    outer_1 = jnp.where(row_id == col_id, edge, outer)
    cat_id = lax.broadcasted_iota(jnp.int32, (A, reach), 0).astype(jnp.float32)
    left, here, right = noted
    sides = [
        (left[0:1, :], left[1:2, :]),
        (here[0:1, :reach], here[1:2, :reach]),
        (here[0:1, reach:], here[1:2, reach:]),
        (right[0:1, :], right[1:2, :]),
    ]
    members = [(annot == cat_id).astype(jnp.bfloat16) for annot, _ in sides]
    scores, chis = [], []
    for half, parts in enumerate(((outer, own_0, mixed), (mixed, own_1, outer_1))):
        at = half * blocks + me
        low, high = [column(ref[pl.ds(at, 1), :]) for ref in bounds[:2]]
        chis.append(bounds[2][pl.ds(at, 1), :])
        start = pl.multiple_of(half * reach + me * share, share)
        chrom = column(here[1:2, pl.ds(start, share)])
        total = jnp.zeros((A, share), jnp.float32)
        for side, corr in enumerate(parts, half):
            square = corr * corr
            adjusted = square - (1.0 - square) / (total_samples - 2)
            ids = first + (side - 1) * reach + col_id
            inside = (ids >= low) & (ids <= high) & (sides[side][1] == chrom)
            rest = jnp.where(inside, adjusted, 0.0)
            for _ in range(3):
                piece = rest.astype(jnp.bfloat16)
                rest = rest - piece.astype(jnp.float32)
                total += lax.dot_general(
                    members[side],
                    piece,
                    (((1,), (1,)), ((), ())),
                    preferred_element_type=jnp.float32,
                )
        scores.append(total)
    score = jnp.concatenate(scores, 1)
    chi = jnp.concatenate(chis, 1)
    weights = 1.0 / jnp.sum(score, 0, keepdims=True)
    weighted = score * weights
    out[:, : 2 * share] = score
    out[:, 2 * share : 2 * share + A] = lax.dot_general(
        weighted,
        score,
        (((1,), (1,)), ((), ())),
        precision=lax.Precision.HIGHEST,
        preferred_element_type=jnp.float32,
    )
    lane = lax.broadcasted_iota(jnp.int32, (A, A), 1)
    plain = jnp.sum(weighted, 1, keepdims=True)
    scaled = jnp.sum(weighted * chi, 1, keepdims=True)
    all_weights = jnp.sum(weights, 1, keepdims=True)
    all_scaled = jnp.sum(weights * chi, 1, keepdims=True)
    out[:, 2 * share + A :] = jnp.where(
        lane == 0,
        plain,
        jnp.where(
            lane == 1,
            scaled,
            jnp.where(lane == 2, all_weights, jnp.where(lane == 3, all_scaled, 0.0)),
        ),
    )


def scored(near, far, noted, bounds, total_samples):
    share = near[0].shape[0] // 3
    operands = [*near, *far, *noted, *bounds]
    return pl.pallas_call(
        functools.partial(score_kernel, total_samples),
        out_shape=jax.ShapeDtypeStruct((A, 2 * share + 2 * A), jnp.float32),
        in_specs=[pl.BlockSpec(memory_space=pltpu.VMEM)] * len(operands),
        out_specs=pl.BlockSpec(memory_space=pltpu.VMEM),
        compiler_params=pltpu.CompilerParams(vmem_limit_bytes=16 * 2**20),
        cost_estimate=pl.CostEstimate(flops=2 * 10**9, bytes_accessed=2 * 10**6, transcendentals=0),
        name="scored",
    )(*operands)


def last_kernel(scale, count, whole, gram, moments, totals):
    gram[...] = scale * whole[:, :A]
    moments[...] = scale * jnp.transpose(whole[:, A:])[0:2, :]
    totals[...] = whole[0:1, A + 2 : A + 4] / count


def finished(whole, scale, count):
    shapes = ((A, A), (2, A), (1, 2))
    return pl.pallas_call(
        functools.partial(last_kernel, scale, count),
        out_shape=tuple(jax.ShapeDtypeStruct(shape, jnp.float32) for shape in shapes),
        in_specs=[pl.BlockSpec(memory_space=pltpu.VMEM)],
        out_specs=(pl.BlockSpec(memory_space=pltpu.VMEM),) * 3,
        compiler_params=pltpu.CompilerParams(vmem_limit_bytes=4 * 2**20),
        name="finished",
    )(whole)


def whole_step(genotypes, win_lo, win_hi, annotation, chromosome, chi_square):
    samp_rows, block_cols = genotypes.shape
    reach = block_cols // 2
    samp_count = lax.axis_size("samp")
    snp_count = lax.axis_size("snp")
    total_samples = samp_rows * samp_count
    snp_total = block_cols * snp_count
    share = reach // samp_count
    me_samp = lax.axis_index("samp")
    cats = A // snp_count

    lower, upper, sums = counted(genotypes)
    raw_right = from_right(lower, "snp")
    raw_left = from_left(upper, "snp")
    sums = samp_total(sums)
    mean_dose = sums[0] / total_samples
    variance = sums[1] / total_samples - mean_dose * mean_dose
    inverse = lax.rsqrt(variance + 1e-05)

    def standard_of(raw, mean, inv):
        return ((raw.astype(jnp.float32) - mean) * inv).astype(jnp.bfloat16)

    notes = jnp.stack(
        [annotation.astype(jnp.float32), chromosome.astype(jnp.float32), mean_dose, inverse]
    )
    z0 = standard_of(lower, mean_dose[:reach], inverse[:reach])
    z1 = standard_of(upper, mean_dose[reach:], inverse[reach:])
    z0, z1 = lax.optimization_barrier((z0, z1))
    a_id = lax.broadcasted_iota(jnp.int32, (reach, reach), 0)
    b_id = lax.broadcasted_iota(jnp.int32, (reach, reach), 1)

    def fixed(part):
        return jnp.round(part * (FIXED / total_samples)).astype(jnp.int16)

    def turned(parts):
        return [
            lax.dynamic_index_in_dim(parts, (me_samp + step) % samp_count, 0, keepdims=False)
            for step in range(samp_count)
        ]

    def shares(square):
        return square.reshape(samp_count, share, reach)

    near = jnp.concatenate(
        [
            shares(fixed(gram_of(z0, z0))),
            shares(fixed(gram_of(z1, z1))),
            shares(fixed(jnp.where(b_id <= a_id, gram_of(z0, z1), gram_of(z1, z0)))),
        ],
        1,
    )
    near = turned(near)
    near = [near[0]] + [shifted(near[step], "samp", step) for step in range(1, samp_count)]
    notes_right = from_right(notes[:, :reach], "snp")
    notes_left = from_left(notes[:, reach:], "snp")

    z_right = standard_of(raw_right, notes_right[2], notes_right[3])
    right_part = gram_of(z1, z_right)
    edge = jnp.sum(jnp.where(a_id == b_id, right_part, 0.0), 0)
    right_part, edge, raw_left, notes_left = lax.optimization_barrier(
        (right_part, edge, raw_left, notes_left)
    )
    z_left = standard_of(raw_left, notes_left[2], notes_left[3])
    edge_rows = jnp.zeros((samp_count, 8, reach), jnp.int16)
    edge_rows = edge_rows.at[:, 0, :share].set(fixed(edge).reshape(samp_count, share))
    far = jnp.concatenate(
        [
            shares(fixed(jnp.where(b_id >= a_id, gram_of(z0, z_left), right_part))),
            edge_rows,
        ],
        1,
    )
    far = turned(far)
    far = [far[0]] + [shifted(far[step], "samp", step) for step in range(1, samp_count)]
    near, far, win_lo, win_hi, chi_square = lax.optimization_barrier(
        (near, far, win_lo, win_hi, chi_square)
    )

    grid_of = lambda vector: vector.reshape(-1, share)
    mine = scored(
        near,
        far,
        (notes_left, notes, notes_right),
        (grid_of(win_lo), grid_of(win_hi), grid_of(chi_square)),
        total_samples,
    )
    mine = mine.reshape(snp_count, cats, 2 * share + 2 * A)
    mine = exchange(mine, "snp")
    sums_part = jnp.sum(mine[:, :, 2 * share :], 0)
    score_part = jnp.moveaxis(mine[:, :, : 2 * share], 0, 1).reshape(cats, -1)
    sums_part = samp_total(sums_part)
    sums_whole = to_all(sums_part, "snp").reshape(A, 2 * A)
    parts = [score_part] + [shifted(score_part, "samp", step) for step in range(1, samp_count)]
    turns = jnp.stack([parts[-turn % samp_count] for turn in range(1, 2 * samp_count)])
    both = lax.dynamic_slice_in_dim(turns, samp_count - 1 - me_samp, samp_count, 0)
    split = both.reshape(samp_count, cats, snp_count, 2, share)
    regrouped = jnp.transpose(split, (1, 2, 3, 0, 4)).reshape(cats, snp_total)
    gram, moments, totals = finished(sums_whole, A / snp_total, snp_total)
    return (regrouped, gram, moments, totals.reshape(2))


def solution(mesh):
    in_specs = (P("samp", "snp"), P("snp"), P("snp"), P("snp"), P("snp"), P("snp"))
    out_specs = (P("snp", None), P(), P(), P())
    return jax.shard_map(whole_step, mesh=mesh, in_specs=in_specs, out_specs=out_specs, check_vma=False)
```
